32 devices in a mesh: parts: 2 (over y), mem: 4 (over z), space: 4 (over x, core).
Axes of the slice: x: 2, y: 2, z: 4, core: 2. Of those that a mesh axis runs over, the one named last changes fastest.
Arguments:
- ensemble: bfloat16 [64, 70, 8192], P('mem', None, ('parts', 'space')), parts along dimension 2, may hold values from -6 to 6
- transform: bfloat16 [128, 64], P('parts'), parts along dimension 0, may hold values from -0.75 to 0.75
- obs_operator: bfloat16 [16, 70], replicated, may hold values from -0.75 to 0.75
- obs_weight: float32 [16, 8192], P(None, ('parts', 'space')), parts along dimension 1, may hold values from 0.25 to 40, as said below
Outputs:
- analysis: bfloat16 [64, 70, 8192], P('mem', None, ('parts', 'space')), parts along dimension 2
- prior_gram: float32 [128, 64], P('parts'), parts along dimension 0
- posterior_gram: float32 [128, 64], P('parts'), parts along dimension 0
The draws below stay inside these ranges and needn't reach their ends.
There are 2 independent parts, one for each index of `parts`. The reference program is written for one: setup_inputs(seed, part) draws one part's arguments, and reference() takes and returns one part's arrays. A program takes and returns all parts, laid end to end along the dimension named above; an argument that names none is the same for every part. Nothing has to cross between parts.
Inputs may be any that keep to these rules, and one draw needn't show every extreme that they name: `obs_weight`: positive.
All inputs are finite; a program needn't handle non-finite values.
Results may differ from the reference program's by a relative error of at most 0.001.
Values may be sent and summed in bfloat16 or wider, within the bound.
A program may use at most 64 MiB of HBM per device.

```python
import math
import jax
import jax.numpy as jnp
from jax import lax

MEMBERS = 64
VARS = 70
OBS = 16
CELLS = 4096


def draw_obs_weight(key, part):
    first_key = jax.random.fold_in(jax.random.fold_in(key, 11), 0)
    levels = jax.random.uniform(first_key, (OBS, CELLS), jnp.float32)
    position = jnp.arange(CELLS, dtype=jnp.float32) / max(CELLS - 1, 1)
    ramp = 1.0 + 2.0 * position
    return 0.5 * jnp.exp(levels * math.log(10.0)) * ramp[None, :]


def level_of(rng, shape, cuts, low, top_value):
    level = 1.0
    for dim, shards_of in cuts:
        steps = jax.random.uniform(jax.random.fold_in(jax.random.fold_in(rng, 6), dim), (shards_of,), jnp.float32, low / len(cuts), top_value / len(cuts))
        level = level * jnp.repeat(jnp.exp(steps), shape[dim] // shards_of).reshape((-1,) + (1,) * (len(shape) - 1 - dim))
    return level


def bell_draw(rng, shape, deviation, reach, shards=(), held_as=jnp.bfloat16):
    array = deviation * jax.random.normal(rng, shape, jnp.float32)
    if shards:
        array = array * level_of(rng, shape, shards, -0.22, 0.18)
    return jnp.clip(array, -reach, reach).astype(held_as)


def setup_inputs(seed: int = 0, part: int = 0) -> dict:
    seeds = jax.random.split(jax.random.key(seed), 5)
    part_splits = jax.random.split(jax.random.fold_in(seeds[4], part), 5)
    ensemble = bell_draw(part_splits[0], (MEMBERS, VARS, CELLS), 1.0, 6.0, ((0, 4), (2, 4)))
    transform = bell_draw(part_splits[1], (MEMBERS, MEMBERS), MEMBERS ** -0.5, 0.75)
    obs_operator = bell_draw(seeds[2], (OBS, VARS), VARS ** -0.5, 0.75)
    obs_weight = draw_obs_weight(jax.random.fold_in(jax.random.fold_in(seeds[4], part), 71), part)
    return dict(ensemble=ensemble, transform=transform, obs_operator=obs_operator, obs_weight=obs_weight)


def reference(ensemble, transform, obs_operator, obs_weight):
    mixing = transform.astype(jnp.float32)
    members = ensemble.astype(jnp.float32)
    member_mean = jnp.sum(members, axis=0) / MEMBERS
    combined = jnp.einsum("ij,ivc->jvc", mixing, members)
    keep_mean = 1.0 - jnp.sum(mixing, axis=0)
    analysis = (combined + member_mean[None, :, :] * keep_mean[:, None, None]).astype(jnp.bfloat16)
    observed = jnp.einsum("ov,mvc->moc", obs_operator.astype(jnp.float32), members)
    departures = observed - jnp.sum(observed, axis=0) / MEMBERS
    weighted = departures * obs_weight[None, :, :]
    gram_sum = jnp.einsum("ioc,joc->ij", weighted, departures, precision=lax.Precision.HIGHEST)
    prior_gram = gram_sum / jnp.sum(obs_weight)
    carried = jnp.dot(mixing.T, prior_gram, precision=lax.Precision.HIGHEST)
    posterior_gram = jnp.dot(carried, mixing, precision=lax.Precision.HIGHEST)
    return analysis, prior_gram, posterior_gram
```

```python
import functools

import jax
import jax.numpy as jnp
from jax import lax
from jax.experimental import pallas as pl
from jax.experimental.pallas import tpu as pltpu
from jax.sharding import PartitionSpec as P

HIGHEST = lax.Precision.HIGHEST
MESH = pl.DeviceIdType.MESH
LANES = 128
PIECE = 14
ROWS = 16
NT = (((1,), (1,)), ((), ()))


def dot(a, b):
    return jnp.dot(a, b, preferred_element_type=jnp.float32)


def selector(shape, match):
    rows = lax.broadcasted_iota(jnp.int32, shape, 0)
    cols = lax.broadcasted_iota(jnp.int32, shape, 1)
    return match(rows, cols)


def as_bf16(mask):
    return jnp.where(mask, 1.0, 0.0).astype(jnp.bfloat16)


def peers_of(me, size):
    if size % 2:
        return [lax.rem(me + step, size) for step in range(1, size)]
    half = size // 2
    side, place = me // half, lax.rem(me, half)
    across = [(1 - side) * half + lax.rem(place + step, half) for step in range(half)]
    return across + [side * half + lax.rem(place + step, half) for step in range(1, half)]


def when(needed, condition, body):
    if needed:
        pl.when(condition)(body)
    else:
        body()


def kernel(
    sizes, ensemble, transform, obs_operator, obs_weight, analysis, prior, posterior,
    arrived, results, observer, observed, gram, by_space, by_mem, in_slabs, out_slabs,
    in_send, in_recv, out_send, out_recv, own_in, own_out,
    space_send, space_recv, mem_send, mem_recv,
):
    n_mem, n_space, active, pieces, local, members, variables, n_obs, chunk = sizes
    blocks = members // ROWS
    aligned = local % ROWS == 0
    partial_owners = active < n_mem
    me = lax.axis_index("mem")
    here = lax.axis_index("space")
    mem_peers = peers_of(me, n_mem)
    space_peers = peers_of(here, n_space)

    def lanes_of(owner):
        return pl.ds(pl.multiple_of(owner * chunk, chunk), chunk)

    def rows_of(device):
        return pl.ds(pl.multiple_of(device * local, local), local)

    barrier = pltpu.get_barrier_semaphore()
    for peer in mem_peers:
        pl.semaphore_signal(barrier, inc=1, device_id={"mem": peer}, device_id_type=MESH)
    for peer in space_peers:
        pl.semaphore_signal(barrier, inc=1, device_id={"space": peer}, device_id_type=MESH)
    pl.semaphore_wait(barrier, n_mem - 1 + n_space - 1)

    def spot(whole, slabs, piece, device):
        start, count = pieces[piece]
        if aligned:
            return whole.at[start : start + count, rows_of(device), :]
        return slabs.at[device, start : start + count]

    def outside(array, piece, owner):
        start, count = pieces[piece]
        return array.at[start : start + count, :, lanes_of(owner)]

    def inward(piece, peer, source):
        return pltpu.make_async_remote_copy(
            src_ref=outside(ensemble, piece, peer),
            dst_ref=spot(arrived, in_slabs, piece, source),
            send_sem=in_send.at[piece, peer],
            recv_sem=in_recv.at[piece, source],
            device_id={"mem": peer},
            device_id_type=MESH,
        )

    def inward_own(piece):
        return pltpu.make_async_copy(
            outside(ensemble, piece, me), spot(arrived, in_slabs, piece, me), own_in.at[piece]
        )

    def outward(piece, peer, owner):
        return pltpu.make_async_remote_copy(
            src_ref=spot(results, out_slabs, piece, peer),
            dst_ref=outside(analysis, piece, owner),
            send_sem=out_send.at[piece, peer],
            recv_sem=out_recv.at[piece, owner],
            device_id={"mem": peer},
            device_id_type=MESH,
        )

    def outward_own(piece):
        return pltpu.make_async_copy(
            spot(results, out_slabs, piece, me), outside(analysis, piece, me), own_out.at[piece]
        )

    owns = me < active
    for piece in range(len(pieces)):
        for peer in mem_peers:
            when(partial_owners, peer < active, lambda: inward(piece, peer, me).start())
        when(partial_owners, owns, lambda: inward_own(piece).start())

    eye = as_bf16(selector((members, members), lambda r, c: r == c))
    mixing_t = lax.dot_general(eye, transform[...], NT, preferred_element_type=jnp.float32)
    keep = 1.0 - jnp.sum(mixing_t, axis=1, keepdims=True)
    ones = jnp.ones((ROWS, members), jnp.float32)
    mixer = jnp.concatenate([mixing_t, ones], axis=0).astype(jnp.bfloat16)

    obs_rows = n_obs * ROWS
    obs_pick = as_bf16(selector((obs_rows, n_obs), lambda r, c: r // ROWS == c))
    for piece, (start, count) in enumerate(pieces):
        depth = count * ROWS
        place = as_bf16(selector((variables, depth), lambda r, c: r == c // ROWS + start))
        part = dot(obs_operator[...], place).astype(jnp.bfloat16)
        mask = selector((obs_rows, depth), lambda r, c: lax.rem(r, ROWS) == lax.rem(c, ROWS))
        full = jnp.where(mask, dot(obs_pick, part), 0.0)
        observer[piece, :, 0:depth] = full.astype(jnp.bfloat16)

    def mix(piece):
        start, count = pieces[piece]
        for variable in range(start, start + count):
            if not aligned:
                for device in range(n_mem):
                    rows = slice(device * local, (device + 1) * local)
                    arrived[variable, rows, :] = in_slabs[device, variable]
            mixed = dot(mixer, arrived[variable])
            mean = mixed[members : members + 1, :] / members
            value = (mixed[:members, :] + keep * mean).astype(jnp.bfloat16)
            if aligned:
                results[variable] = value
            else:
                for device in range(n_mem):
                    rows = slice(device * local, (device + 1) * local)
                    out_slabs[device, variable] = value[rows, :]

    def observe(piece):
        start, count = pieces[piece]
        depth = count * ROWS
        for block in range(blocks):
            at = slice(block * ROWS, (block + 1) * ROWS)
            states = arrived[start : start + count, at, :].reshape(depth, chunk)
            term = dot(observer[piece, :, 0:depth], states).reshape(n_obs, ROWS, chunk)
            if piece == 0:
                observed[:, at, :] = term
            else:
                observed[:, at, :] += term

    def form_gram():
        weights = obs_weight[:, lanes_of(me)]
        total = jnp.zeros((members, members), jnp.float32)
        for quantity in range(n_obs):
            values = observed[quantity]
            departures = values - jnp.sum(values, axis=0, keepdims=True) / members
            total += lax.dot_general(
                departures * weights[quantity : quantity + 1, :],
                departures,
                NT,
                precision=HIGHEST,
                preferred_element_type=jnp.float32,
            )
        gram[0:members, 0:members] = total
        gram[members : members + 8, :] = jnp.full((8, LANES), jnp.sum(weights), jnp.float32)

    gram[...] = jnp.zeros_like(gram)

    def work():
        for piece in range(len(pieces)):
            for peer in mem_peers:
                inward(piece, me, peer).wait_recv()
            inward_own(piece).wait()
            mix(piece)
            for peer in mem_peers:
                outward(piece, peer, me).start()
            outward_own(piece).start()
            observe(piece)
        form_gram()

    when(partial_owners, owns, work)

    def exchange(source, slots, index, peers, axis, send, recv):
        slots[index] = source
        copies = [
            pltpu.make_async_remote_copy(
                src_ref=slots.at[index],
                dst_ref=slots.at[index],
                send_sem=send.at[peer],
                recv_sem=recv.at[index],
                device_id={axis: peer},
                device_id_type=MESH,
            )
            for peer in peers
        ]
        for copy in copies:
            copy.start()
        for peer in peers:
            pltpu.make_async_remote_copy(
                src_ref=slots.at[peer],
                dst_ref=slots.at[peer],
                send_sem=send.at[peer],
                recv_sem=recv.at[peer],
                device_id={axis: peer},
                device_id_type=MESH,
            ).wait_recv()
        total = slots[0]
        for slot in range(1, slots.shape[0]):
            total += slots[slot]
        for copy in copies:
            copy.wait_send()
        return total

    total = exchange(gram[...], by_space, here, space_peers, "space", space_send, space_recv)
    total = exchange(total, by_mem, me, mem_peers, "mem", mem_send, mem_recv)
    prior_gram = total[0:members, 0:members] / total[members : members + 1, 0:members]
    prior[...] = prior_gram
    carried = jnp.dot(
        mixing_t, prior_gram, precision=HIGHEST, preferred_element_type=jnp.float32
    )
    posterior[...] = jnp.dot(
        carried,
        transform[...].astype(jnp.float32),
        precision=HIGHEST,
        preferred_element_type=jnp.float32,
    )

    for piece in range(len(pieces)):
        for peer in mem_peers:
            when(partial_owners, peer < active, lambda: inward(piece, peer, me).wait_send())
            when(partial_owners, owns, lambda: outward(piece, peer, me).wait_send())
            when(partial_owners, peer < active, lambda: outward(piece, me, peer).wait_recv())
        when(partial_owners, owns, lambda: outward_own(piece).wait())


def per_device(n_mem, n_space, ensemble, transform, obs_operator, obs_weight):
    local, variables, cells = ensemble.shape
    members = transform.shape[0]
    n_obs = obs_operator.shape[0]
    active = min(n_mem, cells // LANES)
    chunk = cells // active
    pieces = tuple(
        (start, min(PIECE, variables - start)) for start in range(0, variables, PIECE)
    )
    sizes = (n_mem, n_space, active, pieces, local, members, variables, n_obs, chunk)
    vmem = pl.BlockSpec(memory_space=pltpu.VMEM)
    any_space = pl.BlockSpec(memory_space=pl.ANY)
    gram_shape = (members + 8, LANES)
    slabs = (1, 1, ROWS, LANES) if local % ROWS == 0 else (n_mem, variables, local, chunk)
    dma = pltpu.SemaphoreType.DMA
    by_variable, prior, posterior = pl.pallas_call(
        functools.partial(kernel, sizes),
        out_shape=(
            jax.ShapeDtypeStruct((variables, local, cells), jnp.bfloat16),
            jax.ShapeDtypeStruct((members, members), jnp.float32),
            jax.ShapeDtypeStruct((members, members), jnp.float32),
        ),
        in_specs=[any_space, vmem, vmem, vmem],
        out_specs=(any_space, vmem, vmem),
        scratch_shapes=[
            pltpu.VMEM((variables, members, chunk), jnp.bfloat16),
            pltpu.VMEM((variables, members, chunk), jnp.bfloat16),
            pltpu.VMEM((len(pieces), n_obs * ROWS, PIECE * ROWS), jnp.bfloat16),
            pltpu.VMEM((n_obs, members, chunk), jnp.float32),
            pltpu.VMEM(gram_shape, jnp.float32),
            pltpu.VMEM((n_space,) + gram_shape, jnp.float32),
            pltpu.VMEM((n_mem,) + gram_shape, jnp.float32),
            pltpu.VMEM(slabs, jnp.bfloat16),
            pltpu.VMEM(slabs, jnp.bfloat16),
            dma((len(pieces), n_mem)),
            dma((len(pieces), n_mem)),
            dma((len(pieces), n_mem)),
            dma((len(pieces), n_mem)),
            dma((len(pieces),)),
            dma((len(pieces),)),
            dma((n_space,)),
            dma((n_space,)),
            dma((n_mem,)),
            dma((n_mem,)),
        ],
        compiler_params=pltpu.CompilerParams(collective_id=0, has_side_effects=True),
        name="ensemble_exchange",
    )(jnp.transpose(ensemble, (1, 0, 2)), transform, obs_operator, obs_weight)
    return jnp.transpose(by_variable, (1, 0, 2)), prior, posterior


def solution(mesh):
    return jax.shard_map(
        functools.partial(per_device, mesh.shape["mem"], mesh.shape["space"]),
        mesh=mesh,
        in_specs=(
            P("mem", None, ("parts", "space")),
            P("parts", None),
            P(),
            P(None, ("parts", "space")),
        ),
        out_specs=(P("mem", None, ("parts", "space")), P("parts", None), P("parts", None)),
        check_vma=False,
    )
```

```python
import functools

import jax
import jax.numpy as jnp
from jax import lax
from jax.experimental import pallas as pl
from jax.experimental.pallas import tpu as pltpu
from jax.sharding import PartitionSpec as P

HIGHEST = lax.Precision.HIGHEST
MESH = pl.DeviceIdType.MESH
LANES = 128
PIECE = 14
ROWS = 16
NT = (((1,), (1,)), ((), ()))


def dot(a, b):
    return jnp.dot(a, b, preferred_element_type=jnp.float32)


def selector(shape, match):
    rows = lax.broadcasted_iota(jnp.int32, shape, 0)
    cols = lax.broadcasted_iota(jnp.int32, shape, 1)
    return match(rows, cols)


def as_bf16(mask):
    return jnp.where(mask, 1.0, 0.0).astype(jnp.bfloat16)


def peers_of(me, size):
    if size % 2:
        return [lax.rem(me + step, size) for step in range(1, size)], []
    half = size // 2
    side, place = me // half, lax.rem(me, half)
    across = [(1 - side) * half + lax.rem(place + step, half) for step in range(half)]
    return across, [side * half + lax.rem(place + step, half) for step in range(1, half)]


def when(needed, condition, body):
    if needed:
        pl.when(condition)(body)
    else:
        body()


def kernel(
    sizes, ensemble, *refs,
):
    smalls, refs = refs[:3], refs[3:]
    analysis, prior, posterior, transform, obs_operator, obs_weight, small_sem = refs[:7]
    (
    arrived, results, observer, observed, gram, by_space, by_mem, in_slabs, out_slabs,
    in_send, in_recv, out_send, out_recv, own_in, own_out,
    space_send, space_recv, mem_send, mem_recv,
    ) = refs[7:]
    n_mem, n_space, active, pieces, local, members, variables, n_obs, chunk = sizes
    blocks = members // ROWS
    aligned = local % ROWS == 0
    partial_owners = active < n_mem
    me = lax.axis_index("mem")
    here = lax.axis_index("space")
    across, beside = peers_of(me, n_mem)
    mem_peers = across + beside
    space_peers = sum(peers_of(here, n_space), [])
    central = jnp.logical_or(me * 2 == n_mem, (me + 1) * 2 == n_mem)

    def lanes_of(owner):
        return pl.ds(pl.multiple_of(owner * chunk, chunk), chunk)

    def rows_of(device):
        return pl.ds(pl.multiple_of(device * local, local), local)

    barrier = pltpu.get_barrier_semaphore()
    for peer in mem_peers:
        pl.semaphore_signal(barrier, inc=1, device_id={"mem": peer}, device_id_type=MESH)
    for peer in space_peers:
        pl.semaphore_signal(barrier, inc=1, device_id={"space": peer}, device_id_type=MESH)
    pl.semaphore_wait(barrier, n_mem - 1 + n_space - 1)

    def spot(whole, slabs, piece, device):
        start, count = pieces[piece]
        if aligned:
            return whole.at[start : start + count, rows_of(device), :]
        return slabs.at[device, start : start + count]

    def outside(array, piece, owner):
        start, count = pieces[piece]
        return array.at[start : start + count, :, lanes_of(owner)]

    def inward(piece, peer, source):
        return pltpu.make_async_remote_copy(
            src_ref=outside(ensemble, piece, peer),
            dst_ref=spot(arrived, in_slabs, piece, source),
            send_sem=in_send.at[piece, peer],
            recv_sem=in_recv.at[piece, source],
            device_id={"mem": peer},
            device_id_type=MESH,
        )

    def inward_own(piece):
        return pltpu.make_async_copy(
            outside(ensemble, piece, me), spot(arrived, in_slabs, piece, me), own_in.at[piece]
        )

    def outward(piece, peer, owner):
        return pltpu.make_async_remote_copy(
            src_ref=spot(results, out_slabs, piece, peer),
            dst_ref=outside(analysis, piece, owner),
            send_sem=out_send.at[piece, peer],
            recv_sem=out_recv.at[piece, owner],
            device_id={"mem": peer},
            device_id_type=MESH,
        )

    def outward_own(piece):
        return pltpu.make_async_copy(
            spot(results, out_slabs, piece, me), outside(analysis, piece, me), own_out.at[piece]
        )

    owns = me < active
    for group in (beside, across):
        for piece in range(len(pieces)):
            for peer in group:
                when(partial_owners, peer < active, lambda: inward(piece, peer, me).start())
    for piece in range(len(pieces)):
        when(partial_owners, owns, lambda: inward_own(piece).start())
    loads = [
        pltpu.make_async_copy(source, target, small_sem.at[index])
        for index, (source, target) in enumerate(
            zip(smalls, (transform, obs_operator, obs_weight))
        )
    ]
    for load in loads:
        load.start()
    for load in loads:
        load.wait()

    eye = as_bf16(selector((members, members), lambda r, c: r == c))
    mixing_t = lax.dot_general(eye, transform[...], NT, preferred_element_type=jnp.float32)
    keep = 1.0 - jnp.sum(mixing_t, axis=1, keepdims=True)
    ones = jnp.ones((ROWS, members), jnp.float32)
    mixer = jnp.concatenate([mixing_t, ones], axis=0).astype(jnp.bfloat16)

    obs_rows = n_obs * ROWS
    obs_pick = as_bf16(selector((obs_rows, n_obs), lambda r, c: r // ROWS == c))
    for piece, (start, count) in enumerate(pieces):
        depth = count * ROWS
        place = as_bf16(selector((variables, depth), lambda r, c: r == c // ROWS + start))
        part = dot(obs_operator[...], place).astype(jnp.bfloat16)
        mask = selector((obs_rows, depth), lambda r, c: lax.rem(r, ROWS) == lax.rem(c, ROWS))
        full = jnp.where(mask, dot(obs_pick, part), 0.0)
        observer[piece, :, 0:depth] = full.astype(jnp.bfloat16)

    def mix(piece):
        start, count = pieces[piece]
        for variable in range(start, start + count):
            if not aligned:
                for device in range(n_mem):
                    rows = slice(device * local, (device + 1) * local)
                    arrived[variable, rows, :] = in_slabs[device, variable]
            mixed = dot(mixer, arrived[variable])
            mean = mixed[members : members + 1, :] / members
            value = (mixed[:members, :] + keep * mean).astype(jnp.bfloat16)
            if aligned:
                results[variable] = value
            else:
                for device in range(n_mem):
                    rows = slice(device * local, (device + 1) * local)
                    out_slabs[device, variable] = value[rows, :]

    def observe(piece):
        start, count = pieces[piece]
        depth = count * ROWS
        for block in range(blocks):
            at = slice(block * ROWS, (block + 1) * ROWS)
            states = arrived[start : start + count, at, :].reshape(depth, chunk)
            term = dot(observer[piece, :, 0:depth], states).reshape(n_obs, ROWS, chunk)
            if piece == 0:
                observed[:, at, :] = term
            else:
                observed[:, at, :] += term

    def form_gram():
        weights = obs_weight[:, lanes_of(me)]
        total = jnp.zeros((members, members), jnp.float32)
        for quantity in range(n_obs):
            values = observed[quantity]
            departures = values - jnp.sum(values, axis=0, keepdims=True) / members
            total += lax.dot_general(
                departures * weights[quantity : quantity + 1, :],
                departures,
                NT,
                precision=HIGHEST,
                preferred_element_type=jnp.float32,
            )
        gram[0:members, 0:members] = total
        gram[members : members + 8, :] = jnp.full((8, LANES), jnp.sum(weights), jnp.float32)

    gram[...] = jnp.zeros_like(gram)

    last = len(pieces) - 1

    def send_back(piece, group):
        for peer in group:
            outward(piece, peer, me).start()

    def work():
        for piece in range(last + 1):
            for peer in mem_peers:
                inward(piece, me, peer).wait_recv()
            inward_own(piece).wait()
            mix(piece)
            send_back(piece, beside)
            if piece < last:
                pl.when(central)(lambda: send_back(piece, across))
            outward_own(piece).start()
            observe(piece)
        form_gram()

    def finish_sends():
        for piece in range(last):
            pl.when(jnp.logical_not(central))(lambda: send_back(piece, across))
        send_back(last, across)

    when(partial_owners, owns, work)

    def exchange(source, slots, index, peers, axis, send, recv, between):
        slots[index] = source
        copies = [
            pltpu.make_async_remote_copy(
                src_ref=slots.at[index],
                dst_ref=slots.at[index],
                send_sem=send.at[peer],
                recv_sem=recv.at[index],
                device_id={axis: peer},
                device_id_type=MESH,
            )
            for peer in peers
        ]
        for copy in copies:
            copy.start()
        between()
        for peer in peers:
            pltpu.make_async_remote_copy(
                src_ref=slots.at[peer],
                dst_ref=slots.at[peer],
                send_sem=send.at[peer],
                recv_sem=recv.at[peer],
                device_id={axis: peer},
                device_id_type=MESH,
            ).wait_recv()
        total = slots[0]
        for slot in range(1, slots.shape[0]):
            total += slots[slot]
        for copy in copies:
            copy.wait_send()
        return total

    total = exchange(
        gram[...], by_space, here, space_peers, "space", space_send, space_recv, lambda: None
    )
    total = exchange(
        total, by_mem, me, mem_peers, "mem", mem_send, mem_recv,
        lambda: when(partial_owners, owns, finish_sends),
    )
    prior_gram = total[0:members, 0:members] / total[members : members + 1, 0:members]
    prior[...] = prior_gram
    carried = jnp.dot(
        mixing_t, prior_gram, precision=HIGHEST, preferred_element_type=jnp.float32
    )
    posterior[...] = jnp.dot(
        carried,
        transform[...].astype(jnp.float32),
        precision=HIGHEST,
        preferred_element_type=jnp.float32,
    )

    for piece in range(len(pieces)):
        for peer in mem_peers:
            when(partial_owners, peer < active, lambda: inward(piece, peer, me).wait_send())
            when(partial_owners, owns, lambda: outward(piece, peer, me).wait_send())
            when(partial_owners, peer < active, lambda: outward(piece, me, peer).wait_recv())
        when(partial_owners, owns, lambda: outward_own(piece).wait())


def per_device(n_mem, n_space, ensemble, transform, obs_operator, obs_weight):
    local, variables, cells = ensemble.shape
    members = transform.shape[0]
    n_obs = obs_operator.shape[0]
    active = min(n_mem, cells // LANES)
    chunk = cells // active
    pieces = tuple(
        (start, min(PIECE, variables - start)) for start in range(0, variables, PIECE)
    )
    sizes = (n_mem, n_space, active, pieces, local, members, variables, n_obs, chunk)
    vmem = pl.BlockSpec(memory_space=pltpu.VMEM)
    any_space = pl.BlockSpec(memory_space=pl.ANY)
    gram_shape = (members + 8, LANES)
    slabs = (1, 1, ROWS, LANES) if local % ROWS == 0 else (n_mem, variables, local, chunk)
    dma = pltpu.SemaphoreType.DMA
    by_variable, prior, posterior = pl.pallas_call(
        functools.partial(kernel, sizes),
        out_shape=(
            pltpu.VMEM((variables, local, cells), jnp.bfloat16),
            pltpu.VMEM((members, members), jnp.float32),
            pltpu.VMEM((members, members), jnp.float32),
        ),
        in_specs=[any_space] * 4,
        out_specs=(vmem, vmem, vmem),
        scratch_shapes=[
            pltpu.VMEM(transform.shape, jnp.bfloat16),
            pltpu.VMEM(obs_operator.shape, jnp.bfloat16),
            pltpu.VMEM(obs_weight.shape, jnp.float32),
            dma((3,)),
            pltpu.VMEM((variables, members, chunk), jnp.bfloat16),
            pltpu.VMEM((variables, members, chunk), jnp.bfloat16),
            pltpu.VMEM((len(pieces), n_obs * ROWS, PIECE * ROWS), jnp.bfloat16),
            pltpu.VMEM((n_obs, members, chunk), jnp.float32),
            pltpu.VMEM(gram_shape, jnp.float32),
            pltpu.VMEM((n_space,) + gram_shape, jnp.float32),
            pltpu.VMEM((n_mem,) + gram_shape, jnp.float32),
            pltpu.VMEM(slabs, jnp.bfloat16),
            pltpu.VMEM(slabs, jnp.bfloat16),
            dma((len(pieces), n_mem)),
            dma((len(pieces), n_mem)),
            dma((len(pieces), n_mem)),
            dma((len(pieces), n_mem)),
            dma((len(pieces),)),
            dma((len(pieces),)),
            dma((n_space,)),
            dma((n_space,)),
            dma((n_mem,)),
            dma((n_mem,)),
        ],
        compiler_params=pltpu.CompilerParams(collective_id=0, has_side_effects=True),
        name="ensemble_exchange",
    )(jnp.transpose(ensemble, (1, 0, 2)), transform, obs_operator, obs_weight)
    return jnp.transpose(by_variable, (1, 0, 2)), prior, posterior


def solution(mesh):
    return jax.shard_map(
        functools.partial(per_device, mesh.shape["mem"], mesh.shape["space"]),
        mesh=mesh,
        in_specs=(
            P("mem", None, ("parts", "space")),
            P("parts", None),
            P(),
            P(None, ("parts", "space")),
        ),
        out_specs=(P("mem", None, ("parts", "space")), P("parts", None), P("parts", None)),
        check_vma=False,
    )
```

```python
import functools

import jax
import jax.numpy as jnp
from jax import lax
from jax.experimental import pallas as pl
from jax.experimental.pallas import tpu as pltpu
from jax.sharding import PartitionSpec as P

HIGHEST = lax.Precision.HIGHEST
MESH = pl.DeviceIdType.MESH
LANES = 128
PIECE = 14
ROWS = 16
NT = (((1,), (1,)), ((), ()))


def dot(a, b):
    return jnp.dot(a, b, preferred_element_type=jnp.float32)


def selector(shape, match):
    rows = lax.broadcasted_iota(jnp.int32, shape, 0)
    cols = lax.broadcasted_iota(jnp.int32, shape, 1)
    return match(rows, cols)


def as_bf16(mask):
    return jnp.where(mask, 1.0, 0.0).astype(jnp.bfloat16)


def peers_of(me, size):
    if size % 2:
        return [lax.rem(me + step, size) for step in range(1, size)], []
    half = size // 2
    side, place = me // half, lax.rem(me, half)
    across = [(1 - side) * half + lax.rem(place + step, half) for step in range(half)]
    return across, [side * half + lax.rem(place + step, half) for step in range(1, half)]


def when(needed, condition, body):
    if needed:
        pl.when(condition)(body)
    else:
        body()


def kernel(
    sizes, ensemble, *refs,
):
    smalls, refs = refs[:3], refs[3:]
    analysis, prior, posterior, transform, obs_operator, obs_weight, small_sem = refs[:7]
    (
    arrived, results, observer, observed, gram, by_space, by_mem, in_slabs, out_slabs,
    in_send, in_recv, out_send, out_recv, own_in, own_out,
    space_send, space_recv, mem_send, mem_recv,
    ) = refs[7:]
    n_mem, n_space, active, pieces, local, members, variables, n_obs, chunk = sizes
    blocks = members // ROWS
    aligned = local % ROWS == 0
    partial_owners = active < n_mem
    me = lax.axis_index("mem")
    here = lax.axis_index("space")
    across, beside = peers_of(me, n_mem)
    mem_peers = across + beside
    space_peers = sum(peers_of(here, n_space), [])
    central = jnp.logical_or(me * 2 == n_mem, (me + 1) * 2 == n_mem)

    def lanes_of(owner):
        return pl.ds(pl.multiple_of(owner * chunk, chunk), chunk)

    def rows_of(device):
        return pl.ds(pl.multiple_of(device * local, local), local)

    barrier = pltpu.get_barrier_semaphore()
    for peer in mem_peers:
        pl.semaphore_signal(barrier, inc=1, device_id={"mem": peer}, device_id_type=MESH)
    for peer in space_peers:
        pl.semaphore_signal(barrier, inc=1, device_id={"space": peer}, device_id_type=MESH)
    pl.semaphore_wait(barrier, n_mem - 1 + n_space - 1)

    def spot(whole, slabs, piece, device):
        start, count = pieces[piece]
        if aligned:
            return whole.at[start : start + count, rows_of(device), :]
        return slabs.at[device, start : start + count]

    def outside(array, piece, owner):
        start, count = pieces[piece]
        return array.at[start : start + count, :, lanes_of(owner)]

    def inward(piece, peer, source):
        return pltpu.make_async_remote_copy(
            src_ref=outside(ensemble, piece, peer),
            dst_ref=spot(arrived, in_slabs, piece, source),
            send_sem=in_send.at[piece, peer],
            recv_sem=in_recv.at[piece, source],
            device_id={"mem": peer},
            device_id_type=MESH,
        )

    def inward_own(piece):
        return pltpu.make_async_copy(
            outside(ensemble, piece, me), spot(arrived, in_slabs, piece, me), own_in.at[piece]
        )

    def outward(piece, peer, owner):
        return pltpu.make_async_remote_copy(
            src_ref=spot(results, out_slabs, piece, peer),
            dst_ref=outside(analysis, piece, owner),
            send_sem=out_send.at[piece, peer],
            recv_sem=out_recv.at[piece, owner],
            device_id={"mem": peer},
            device_id_type=MESH,
        )

    def outward_own(piece):
        return pltpu.make_async_copy(
            spot(results, out_slabs, piece, me), outside(analysis, piece, me), own_out.at[piece]
        )

    owns = me < active
    for group in (beside, across):
        for piece in range(len(pieces)):
            for peer in group:
                when(partial_owners, peer < active, lambda: inward(piece, peer, me).start())
    for piece in range(len(pieces)):
        when(partial_owners, owns, lambda: inward_own(piece).start())
    loads = [
        pltpu.make_async_copy(source, target, small_sem.at[index])
        for index, (source, target) in enumerate(
            zip(smalls, (transform, obs_operator, obs_weight))
        )
    ]
    for load in loads:
        load.start()
    for load in loads:
        load.wait()

    eye = as_bf16(selector((members, members), lambda r, c: r == c))
    mixing_t = lax.dot_general(eye, transform[...], NT, preferred_element_type=jnp.float32)
    keep = 1.0 - jnp.sum(mixing_t, axis=1, keepdims=True)
    ones = jnp.ones((ROWS, members), jnp.float32)
    mixer = jnp.concatenate([mixing_t, ones], axis=0).astype(jnp.bfloat16)

    obs_rows = n_obs * ROWS
    obs_pick = as_bf16(selector((obs_rows, n_obs), lambda r, c: r // ROWS == c))
    for piece, (start, count) in enumerate(pieces):
        depth = count * ROWS
        place = as_bf16(selector((variables, depth), lambda r, c: r == c // ROWS + start))
        part = dot(obs_operator[...], place).astype(jnp.bfloat16)
        mask = selector((obs_rows, depth), lambda r, c: lax.rem(r, ROWS) == lax.rem(c, ROWS))
        full = jnp.where(mask, dot(obs_pick, part), 0.0)
        observer[piece, :, 0:depth] = full.astype(jnp.bfloat16)

    def mix(piece):
        start, count = pieces[piece]
        for variable in range(start, start + count):
            if not aligned:
                for device in range(n_mem):
                    rows = slice(device * local, (device + 1) * local)
                    arrived[variable, rows, :] = in_slabs[device, variable]
            mixed = dot(mixer, arrived[variable])
            mean = mixed[members : members + 1, :] / members
            value = (mixed[:members, :] + keep * mean).astype(jnp.bfloat16)
            if aligned:
                results[variable] = value
            else:
                for device in range(n_mem):
                    rows = slice(device * local, (device + 1) * local)
                    out_slabs[device, variable] = value[rows, :]

    def observe(piece):
        start, count = pieces[piece]
        depth = count * ROWS
        for block in range(blocks):
            at = slice(block * ROWS, (block + 1) * ROWS)
            states = arrived[start : start + count, at, :].reshape(depth, chunk)
            term = dot(observer[piece, :, 0:depth], states).reshape(n_obs, ROWS, chunk)
            if piece == 0:
                observed[:, at, :] = term
            else:
                observed[:, at, :] += term

    def form_gram():
        weights = obs_weight[:, lanes_of(me)]
        total = jnp.zeros((members, members), jnp.float32)
        for quantity in range(n_obs):
            values = observed[quantity]
            departures = values - jnp.sum(values, axis=0, keepdims=True) / members
            total += lax.dot_general(
                departures * weights[quantity : quantity + 1, :],
                departures,
                NT,
                precision=HIGHEST,
                preferred_element_type=jnp.float32,
            )
        gram[0:members, 0:members] = total
        gram[members : members + 8, :] = jnp.full((8, LANES), jnp.sum(weights), jnp.float32)

    gram[...] = jnp.zeros_like(gram)

    last = len(pieces) - 1

    def send_back(piece, group):
        for peer in group:
            outward(piece, peer, me).start()

    def work():
        for piece in range(last + 1):
            for peer in mem_peers:
                inward(piece, me, peer).wait_recv()
            inward_own(piece).wait()
            mix(piece)
            send_back(piece, beside)
            if piece < last:
                pl.when(central)(lambda: send_back(piece, across))
            outward_own(piece).start()
            observe(piece)
        form_gram()

    def finish_sends():
        for piece in range(last):
            pl.when(jnp.logical_not(central))(lambda: send_back(piece, across))
        send_back(last, across)

    when(partial_owners, owns, work)

    def exchange(source, slots, index, peers, axis, send, recv, between):
        slots[index] = source
        copies = [
            pltpu.make_async_remote_copy(
                src_ref=slots.at[index],
                dst_ref=slots.at[index],
                send_sem=send.at[peer],
                recv_sem=recv.at[index],
                device_id={axis: peer},
                device_id_type=MESH,
            )
            for peer in peers
        ]
        for copy in copies:
            copy.start()
        between()
        for peer in peers:
            pltpu.make_async_remote_copy(
                src_ref=slots.at[peer],
                dst_ref=slots.at[peer],
                send_sem=send.at[peer],
                recv_sem=recv.at[peer],
                device_id={axis: peer},
                device_id_type=MESH,
            ).wait_recv()
        total = slots[0]
        for slot in range(1, slots.shape[0]):
            total += slots[slot]
        for copy in copies:
            copy.wait_send()
        return total

    total = exchange(
        gram[...], by_space, here, space_peers, "space", space_send, space_recv, lambda: None
    )
    total = exchange(
        total, by_mem, me, mem_peers, "mem", mem_send, mem_recv,
        lambda: when(partial_owners, owns, finish_sends),
    )
    prior_gram = total[0:members, 0:members] / total[members : members + 1, 0:members]
    prior[...] = prior_gram
    carried = jnp.dot(
        mixing_t, prior_gram, precision=HIGHEST, preferred_element_type=jnp.float32
    )
    posterior[...] = jnp.dot(
        carried,
        transform[...].astype(jnp.float32),
        precision=HIGHEST,
        preferred_element_type=jnp.float32,
    )

    for piece in range(len(pieces)):
        for peer in mem_peers:
            when(partial_owners, peer < active, lambda: inward(piece, peer, me).wait_send())
            when(partial_owners, owns, lambda: outward(piece, peer, me).wait_send())
            when(partial_owners, peer < active, lambda: outward(piece, me, peer).wait_recv())
        when(partial_owners, owns, lambda: outward_own(piece).wait())


def store(*refs):
    count = len(refs) // 2
    sources, targets, sems = refs[:count], refs[count : 2 * count], refs[-1]
    pairs = []
    for source, target in zip(sources, targets):
        if len(source.shape) == 3:
            for start in range(0, source.shape[0], PIECE):
                part = slice(start, min(start + PIECE, source.shape[0]))
                pairs.append((source.at[part], target.at[part]))
        else:
            pairs.append((source, target))
    copies = [
        pltpu.make_async_copy(source, target, sems.at[index])
        for index, (source, target) in enumerate(pairs)
    ]
    for copy in copies:
        copy.start()
    for copy in copies:
        copy.wait()


def write_out(*arrays):
    return pl.pallas_call(
        store,
        out_shape=tuple(jax.ShapeDtypeStruct(a.shape, a.dtype) for a in arrays),
        in_specs=[pl.BlockSpec(memory_space=pl.ANY)] * len(arrays),
        out_specs=tuple([pl.BlockSpec(memory_space=pl.ANY)] * len(arrays)),
        scratch_shapes=[pltpu.SemaphoreType.DMA((len(arrays) + pl.cdiv(arrays[0].shape[0], PIECE),))],
        compiler_params=pltpu.CompilerParams(vmem_limit_bytes=8 << 20),
        name="store_outputs",
    )(*arrays)


def per_device(n_mem, n_space, ensemble, transform, obs_operator, obs_weight):
    local, variables, cells = ensemble.shape
    members = transform.shape[0]
    n_obs = obs_operator.shape[0]
    active = min(n_mem, cells // LANES)
    chunk = cells // active
    pieces = tuple(
        (start, min(PIECE, variables - start)) for start in range(0, variables, PIECE)
    )
    sizes = (n_mem, n_space, active, pieces, local, members, variables, n_obs, chunk)
    vmem = pl.BlockSpec(memory_space=pltpu.VMEM)
    any_space = pl.BlockSpec(memory_space=pl.ANY)
    gram_shape = (members + 8, LANES)
    slabs = (1, 1, ROWS, LANES) if local % ROWS == 0 else (n_mem, variables, local, chunk)
    dma = pltpu.SemaphoreType.DMA
    by_variable, prior, posterior = pl.pallas_call(
        functools.partial(kernel, sizes),
        out_shape=(
            pltpu.VMEM((variables, local, cells), jnp.bfloat16),
            pltpu.VMEM((members, members), jnp.float32),
            pltpu.VMEM((members, members), jnp.float32),
        ),
        in_specs=[any_space] * 4,
        out_specs=(vmem, vmem, vmem),
        scratch_shapes=[
            pltpu.VMEM(transform.shape, jnp.bfloat16),
            pltpu.VMEM(obs_operator.shape, jnp.bfloat16),
            pltpu.VMEM(obs_weight.shape, jnp.float32),
            dma((3,)),
            pltpu.VMEM((variables, members, chunk), jnp.bfloat16),
            pltpu.VMEM((variables, members, chunk), jnp.bfloat16),
            pltpu.VMEM((len(pieces), n_obs * ROWS, PIECE * ROWS), jnp.bfloat16),
            pltpu.VMEM((n_obs, members, chunk), jnp.float32),
            pltpu.VMEM(gram_shape, jnp.float32),
            pltpu.VMEM((n_space,) + gram_shape, jnp.float32),
            pltpu.VMEM((n_mem,) + gram_shape, jnp.float32),
            pltpu.VMEM(slabs, jnp.bfloat16),
            pltpu.VMEM(slabs, jnp.bfloat16),
            dma((len(pieces), n_mem)),
            dma((len(pieces), n_mem)),
            dma((len(pieces), n_mem)),
            dma((len(pieces), n_mem)),
            dma((len(pieces),)),
            dma((len(pieces),)),
            dma((n_space,)),
            dma((n_space,)),
            dma((n_mem,)),
            dma((n_mem,)),
        ],
        compiler_params=pltpu.CompilerParams(collective_id=0, has_side_effects=True),
        name="ensemble_exchange",
    )(jnp.transpose(ensemble, (1, 0, 2)), transform, obs_operator, obs_weight)
    by_variable, prior, posterior = write_out(by_variable, prior, posterior)
    return jnp.transpose(by_variable, (1, 0, 2)), prior, posterior


def solution(mesh):
    return jax.shard_map(
        functools.partial(per_device, mesh.shape["mem"], mesh.shape["space"]),
        mesh=mesh,
        in_specs=(
            P("mem", None, ("parts", "space")),
            P("parts", None),
            P(),
            P(None, ("parts", "space")),
        ),
        out_specs=(P("mem", None, ("parts", "space")), P("parts", None), P("parts", None)),
        check_vma=False,
    )
```
